128 devices in a mesh: py: 4 (over y), px: 4 (over z), pz: 8 (over x, core).
Axes of the slice: x: 4, y: 4, z: 4, core: 2. Of those that a mesh axis runs over, the one named last changes fastest.
Arguments:
- field_now: float32 [16, 512, 256, 128], P('py', 'px', 'pz'), may hold values from 0.5 to 2
- earlier: float32 [16, 512, 256, 128], P('py', 'px', 'pz'), may hold values from 0.2 to 1.8
- speed_square: float32 [16, 512, 256, 128], P('py', 'px', 'pz'), may hold values from 0.05 to 0.3
Outputs:
- anomaly: float32 [16, 512, 256, 128], P('py', 'px', 'pz')
- field_now_end: float32 [16, 512, 256, 128], P('py', 'px', 'pz')
The draws below stay inside these ranges and needn't reach their ends.
All inputs are finite; a program needn't handle non-finite values.
Results may differ from the reference program's by a relative error of at most 0.00002.
Values sent between devices are 32-bit elements; how exact they have to be, the bound alone decides.
A program may use at most 128 MiB of HBM per device.

```python
import jax
import jax.numpy as jnp
from jax import lax

GRID_J = 16
GRID_I = 512
GRID_K = 256
LEVELS = 128
STEPS = 4


def shard_levels(key, extent, pieces, smallest, high):
    factor_of, own = 1.0, jax.random.fold_in(key, 6)
    for dim, blocks in pieces:
        draws = jnp.exp(jax.random.uniform(jax.random.fold_in(own, dim), (blocks,), jnp.float32, smallest / len(pieces), high / len(pieces)))
        factor_of = factor_of * jnp.repeat(draws, extent[dim] // blocks).reshape([-1 if axis == dim else 1 for axis in range(len(extent))])
    return factor_of


def setup_inputs(seed: int = 0) -> dict:
    streams_of = jax.random.split(jax.random.key(seed), 4)
    return {
        "field_now": jnp.clip(0.5 + 1.5 * jax.random.uniform(streams_of[0], (GRID_J, GRID_I, GRID_K, LEVELS), jnp.float32) ** shard_levels(streams_of[0], (GRID_J, GRID_I, GRID_K, LEVELS), ((0, 4), (1, 4), (2, 8)), -0.2, 0.2), 0.5, 2.0),
        "earlier": jnp.clip(0.2 + 1.5999999 * jax.random.uniform(streams_of[1], (GRID_J, GRID_I, GRID_K, LEVELS), jnp.float32) ** shard_levels(streams_of[1], (GRID_J, GRID_I, GRID_K, LEVELS), ((0, 4), (1, 4), (2, 8)), -0.2, 0.2), 0.2, 1.8),
        "speed_square": jnp.clip(0.05 + 0.25 * jax.random.uniform(streams_of[2], (GRID_J, GRID_I, GRID_K, LEVELS), jnp.float32) ** shard_levels(streams_of[2], (GRID_J, GRID_I, GRID_K, LEVELS), ((0, 4), (1, 4), (2, 8)), -0.2, 0.2), 0.05, 0.3),
    }


def inner_cells(values, dims):
    for dim in dims:
        values = lax.slice_in_dim(values, 1, values.shape[dim] - 1, axis=dim)
    return values

def side_cells(values, dim, start, dims):
    others = [other for other in dims if other != dim]
    values = inner_cells(values, others)
    return lax.slice_in_dim(values, start, start + values.shape[dim] - 2, axis=dim)

def advance(padded, before, speed_square):
    middle = inner_cells(padded, (0, 1, 2))
    lower = [side_cells(padded, dim, 0, (0, 1, 2)) for dim in (0, 1, 2)]
    upper = [side_cells(padded, dim, 2, (0, 1, 2)) for dim in (0, 1, 2)]
    spread = lower[0] + upper[0] + lower[1] + upper[1] + lower[2] + upper[2] - 6.0 * middle
    return 2.0 * middle - before + speed_square * spread

def reference(field_now, earlier, speed_square):
    for step in range(STEPS):
        later = advance(jnp.pad(field_now, ((1, 1), (1, 1), (1, 1), (0, 0)), mode='constant'), earlier, speed_square)
        earlier, field_now = (field_now, later)
    line_mean = lax.optimization_barrier(jnp.mean(field_now, axis=1, keepdims=True))
    centred = field_now - line_mean
    line_variance = lax.optimization_barrier(jnp.mean(centred * centred, axis=1, keepdims=True))
    anomaly = centred * lax.rsqrt(line_variance + 0.0001)
    return (anomaly, field_now)
```

```python
import functools

import jax
import jax.numpy as jnp
from jax import lax
from jax.experimental import pallas as pl
from jax.experimental.pallas import tpu as pltpu
from jax.sharding import PartitionSpec as P

STEPS = 4
CHUNKS = 8
MESH = pl.DeviceIdType.MESH
PAD = 8


def leapfrog(dims, f_hbm, e_hbm, c_hbm, out, stat, fld, csq, acc, gath, jsend, jrecv, ksend, krecv, isend, irecv, tsend, trecv, local):
    nj, ni, nk, npy, npx, npz = dims
    rows = ni // CHUNKS
    y, x, z = lax.axis_index("py"), lax.axis_index("px"), lax.axis_index("pz")
    k0, k1 = PAD, PAD + nk
    inner = pl.ds(k0, nk)
    sides = {"py": (y, npy), "px": (x, npx), "pz": (z, npz)}

    def has(axis, side):
        index, count = sides[axis]
        return index > 0 if side == 0 else index < count - 1

    def beside(axis, side):
        return {axis: sides[axis][0] + (2 * side - 1)}

    def load_faces(m, side):
        return pltpu.make_async_copy(
            f_hbm.at[(nj - 1) * side, pl.ds(m * rows, rows)],
            fld.at[0, 1 + (nj - 1) * side, pl.ds(1 + m * rows, rows), inner],
            local.at[side, m],
        )

    def load_inner(m):
        return pltpu.make_async_copy(
            f_hbm.at[pl.ds(1, nj - 2), pl.ds(m * rows, rows)],
            fld.at[0, pl.ds(2, nj - 2), pl.ds(1 + m * rows, rows), inner],
            local.at[2, m],
        )

    def load_earlier(m):
        return pltpu.make_async_copy(
            e_hbm.at[:, pl.ds(m * rows, rows)],
            fld.at[1, pl.ds(1, nj), pl.ds(1 + m * rows, rows), inner],
            local.at[3, m],
        )

    def load_speed(m):
        return pltpu.make_async_copy(c_hbm.at[:, pl.ds(m * rows, rows)], csq.at[:, pl.ds(m * rows, rows)], local.at[4, m])

    def plane(p, m, side):
        span = pl.ds(1 + m * rows, rows)
        return pltpu.make_async_remote_copy(
            fld.at[p, 1 + (nj - 1) * side, span, inner],
            fld.at[p, (nj + 1) * (1 - side), span, inner],
            jsend.at[p, side, m], jrecv.at[p, 1 - side, m],
            device_id=beside("py", side), device_id_type=MESH,
        )

    def edge_k(p, m, side):
        span = pl.ds(1 + m * rows, rows)
        return pltpu.make_async_remote_copy(
            fld.at[p, pl.ds(1, nj), span, pl.ds((k1 - 1) if side else k0, 1)],
            fld.at[p, pl.ds(1, nj), span, pl.ds((k0 - 1) if side else k1, 1)],
            ksend.at[p, side, m], krecv.at[p, 1 - side, m],
            device_id=beside("pz", side), device_id_type=MESH,
        )

    def edge_i(p, side):
        return pltpu.make_async_remote_copy(
            fld.at[p, pl.ds(1, nj), ni if side else 1, inner],
            fld.at[p, pl.ds(1, nj), 0 if side else ni + 1, inner],
            isend.at[p, side], irecv.at[p, 1 - side],
            device_id=beside("px", side), device_id_type=MESH,
        )

    def wait_from(copy):
        copy.wait_recv()

    def each_side(axis, do):
        for side in (0, 1):
            pl.when(has(axis, side))(functools.partial(do, side))

    def over_chunks(do):
        def body(m, _):
            do(m)
            return 0
        lax.fori_loop(0, CHUNKS, body, 0)

    def start_loads(m):
        load_faces(m, 0).start()
        load_faces(m, 1).start()

    over_chunks(start_loads)

    def start_rest(m):
        load_inner(m).start()
        load_earlier(m).start()
        load_speed(m).start()

    over_chunks(start_rest)

    barrier = pltpu.get_barrier_semaphore()
    expected = jnp.int32(npx - 1)
    for axis in ("py", "pz"):
        for side in (0, 1):
            expected = expected + has(axis, side).astype(jnp.int32)

            @pl.when(has(axis, side))
            def _(axis=axis, side=side):
                pl.semaphore_signal(barrier, inc=1, device_id=beside(axis, side), device_id_type=MESH)

    for hop in range(1, npx):
        pl.semaphore_signal(barrier, inc=1, device_id={"px": lax.rem(x + hop, npx)}, device_id_type=MESH)
    pl.semaphore_wait(barrier, expected)

    def first_planes(m):
        load_faces(m, 0).wait()
        load_faces(m, 1).wait()
        each_side("py", lambda side: plane(0, m, side).start())

    over_chunks(first_planes)

    def first_edges(m):
        load_inner(m).wait()
        each_side("pz", lambda side: edge_k(0, m, side).start())

    over_chunks(first_edges)
    each_side("px", lambda side: edge_i(0, side).start())

    for side in (0, 1):
        @pl.when(jnp.logical_not(has("py", side)))
        def _(side=side):
            def clear(i, _):
                for p in (0, 1):
                    fld[p, (nj + 1) * side, i + 1, k0:k1] = jnp.zeros((nk, fld.shape[-1]), jnp.float32)
                return 0
            lax.fori_loop(0, ni, clear, 0)

        @pl.when(jnp.logical_not(has("px", side)))
        def _(side=side):
            for p in (0, 1):
                for j in range(nj):
                    fld[p, j + 1, (ni + 1) * side, k0:k1] = jnp.zeros((nk, fld.shape[-1]), jnp.float32)

        @pl.when(jnp.logical_not(has("pz", side)))
        def _(side=side):
            at = k1 if side else k0 - 8
            def clear(i, _):
                for p in (0, 1):
                    for j in range(nj):
                        fld[p, j + 1, i + 1, at:at + 8] = jnp.zeros((8, fld.shape[-1]), jnp.float32)
                return 0
            lax.fori_loop(0, ni, clear, 0)

    def advance(s, m):
        p, q = s % 2, 1 - s % 2
        last = s == STEPS - 1
        first = m * rows
        for j in range(nj):
            if last:
                shift = fld[p, j + 1, 1, k0:k1]

            def row(r, carry):
                before, middle = carry[:2]
                i = first + r + 1
                after = fld[p, j + 1, i + 1, k0:k1]
                along_j = fld[p, j, i, k0:k1] + fld[p, j + 2, i, k0:k1]
                along_k = fld[p, j + 1, i, k0 - 1:k1 - 1] + fld[p, j + 1, i, k0 + 1:k1 + 1]
                spread = (along_j + (before + after)) + along_k - 6.0 * middle
                later = 2.0 * middle - fld[q, j + 1, i, k0:k1] + csq[j, i - 1] * spread
                if not last:
                    fld[q, j + 1, i, k0:k1] = later
                    return middle, after
                out[j, i - 1] = later
                moved = later - shift
                return middle, after, carry[2] + moved, carry[3] + moved * moved

            carry = (fld[p, j + 1, first, k0:k1], fld[p, j + 1, first + 1, k0:k1])
            if last:
                carry = carry + (acc[0, j], acc[1, j])
            carry = lax.fori_loop(0, rows, row, carry, unroll=4)
            if last:
                acc[0, j] = carry[2]
                acc[1, j] = carry[3]

    acc[...] = jnp.zeros_like(acc)
    for s in range(STEPS):
        p, q = s % 2, 1 - s % 2

        def chunk(m, s=s, p=p, q=q):
            if s == 0:
                load_earlier(m).wait()
                load_speed(m).wait()
            each_side("pz", lambda side: edge_k(p, m, 1 - side).wait_recv())
            for side, at in ((0, 0), (1, CHUNKS - 1)):
                @pl.when(jnp.logical_and(has("px", side), m == at))
                def _(side=side):
                    edge_i(p, 1 - side).wait_recv()
            if s > 0:
                each_side("py", lambda side: plane(q, m, side).wait_send())
                each_side("pz", lambda side: edge_k(q, m, side).wait_send())
                for side, at in ((0, 0), (1, CHUNKS - 1)):
                    @pl.when(jnp.logical_and(has("px", side), m == at))
                    def _(side=side):
                        edge_i(q, side).wait_send()
            each_side("py", lambda side: plane(p, m, 1 - side).wait_recv())
            advance(s, m)
            if s < STEPS - 1:
                each_side("py", lambda side: plane(q, m, side).start())
                each_side("pz", lambda side: edge_k(q, m, side).start())
                for side, at in ((0, 0), (1, CHUNKS - 1)):
                    @pl.when(jnp.logical_and(has("px", side), m == at))
                    def _(side=side):
                        edge_i(q, side).start()

        over_chunks(chunk)

    shift = fld[(STEPS - 1) % 2, 1:1 + nj, 1, k0:k1]
    mean = acc[0] * (1.0 / ni)
    gath[x, 0] = shift + mean
    gath[x, 1] = acc[1] - acc[0] * mean

    def totals(hop):
        return pltpu.make_async_remote_copy(
            gath.at[x], gath.at[x], tsend.at[hop - 1], trecv.at[hop - 1],
            device_id={"px": lax.rem(x + hop, npx)}, device_id_type=MESH,
        )

    for hop in range(1, npx):
        totals(hop).start()
    p = (STEPS - 1) % 2

    def finish(m):
        each_side("py", lambda side: plane(p, m, side).wait_send())
        each_side("pz", lambda side: edge_k(p, m, side).wait_send())

    over_chunks(finish)
    each_side("px", lambda side: edge_i(p, side).wait_send())
    for hop in range(1, npx):
        totals(hop).wait()
    whole = gath[0, 0]
    for n in range(1, npx):
        whole = whole + gath[n, 0]
    whole = whole * (1.0 / npx)
    squares = jnp.zeros_like(whole)
    for n in range(npx):
        off = gath[n, 0] - whole
        squares = squares + (gath[n, 1] + ni * (off * off))
    stat[0] = whole
    stat[1] = lax.rsqrt(squares * (1.0 / (ni * npx)) + 0.0001)


def normalise(f_ref, stat_ref, anomaly_hbm, end_hbm, staged, sems, end_sem):
    nj, ni = f_ref.shape[:2]
    rows = ni // CHUNKS
    ends = [pltpu.make_async_copy(f_ref.at[j], end_hbm.at[j], end_sem.at[j]) for j in range(nj)]
    for copy in ends:
        copy.start()

    def leave(m):
        return pltpu.make_async_copy(
            staged.at[:, pl.ds(m * rows, rows)], anomaly_hbm.at[:, pl.ds(m * rows, rows)], sems.at[m]
        )

    def chunk(m, _):
        for j in range(nj):
            mean, scale = stat_ref[0, j], stat_ref[1, j]

            def row(r, _):
                staged[j, m * rows + r] = (f_ref[j, m * rows + r] - mean) * scale
                return 0

            lax.fori_loop(0, rows, row, 0, unroll=4)
        leave(m).start()
        return 0

    lax.fori_loop(0, CHUNKS, chunk, 0)

    def done(m, _):
        leave(m).wait()
        return 0

    lax.fori_loop(0, CHUNKS, done, 0)
    for copy in ends:
        copy.wait()


def solution(mesh):
    npy, npx, npz = (mesh.shape[a] for a in ("py", "px", "pz"))

    def shards(field_now, earlier, speed_square):
        nj, ni, nk, nl = field_now.shape
        f32 = jnp.float32
        dma = pltpu.SemaphoreType.DMA
        hbm = pl.BlockSpec(memory_space=pltpu.HBM)
        vmem = pl.BlockSpec(memory_space=pltpu.VMEM)
        end, stat = pl.pallas_call(
            functools.partial(leapfrog, (nj, ni, nk, npy, npx, npz)),
            out_shape=(pltpu.VMEM((nj, ni, nk, nl), f32), pltpu.VMEM((2, nj, nk, nl), f32)),
            in_specs=[hbm] * 3,
            out_specs=(vmem, vmem),
            scratch_shapes=[
                pltpu.VMEM((2, nj + 2, ni + 2, nk + 2 * PAD, nl), f32),
                pltpu.VMEM((nj, ni, nk, nl), f32),
                pltpu.VMEM((2, nj, nk, nl), f32),
                pltpu.VMEM((npx, 2, nj, nk, nl), f32),
                dma((2, 2, CHUNKS)), dma((2, 2, CHUNKS)),
                dma((2, 2, CHUNKS)), dma((2, 2, CHUNKS)),
                dma((2, 2)), dma((2, 2)),
                dma((npx - 1,)), dma((npx - 1,)),
                dma((5, CHUNKS)),
            ],
            compiler_params=pltpu.CompilerParams(
                collective_id=0, has_side_effects=True, vmem_limit_bytes=48 << 20
            ),
            name="leapfrog",
        )(field_now, earlier, speed_square)
        return pl.pallas_call(
            normalise,
            out_shape=(jax.ShapeDtypeStruct((nj, ni, nk, nl), f32),) * 2,
            in_specs=[vmem, vmem],
            out_specs=(hbm, hbm),
            scratch_shapes=[pltpu.VMEM((nj, ni, nk, nl), f32), dma((CHUNKS,)), dma((nj,))],
            compiler_params=pltpu.CompilerParams(vmem_limit_bytes=20 << 20),
            name="normalise",
        )(end, stat)

    spec = P("py", "px", "pz", None)
    return jax.shard_map(shards, mesh=mesh, in_specs=(spec,) * 3, out_specs=(spec,) * 2, check_vma=False)
```

```python
import functools

import jax
import jax.numpy as jnp
from jax import lax
from jax.experimental import pallas as pl
from jax.experimental.pallas import tpu as pltpu
from jax.sharding import PartitionSpec as P

STEPS = 4
CHUNKS = 8
SPANS = 4
TILE = 8
MESH = pl.DeviceIdType.MESH
PAD = 8


def leapfrog(dims, f_hbm, e_hbm, c_hbm, out, stat, fld, csq, acc, inner_sums, face_sums, jsend, jrecv, lsend, lrecv, ksend, krecv, isend, irecv, tsend, trecv, local):
    nj, ni, nk, npy, npx, npz = dims
    rows, long = ni // CHUNKS, ni // SPANS
    tiles = nk // TILE
    final = (STEPS - 1) % 2
    y, x, z = lax.axis_index("py"), lax.axis_index("px"), lax.axis_index("pz")
    k0, k1 = PAD, PAD + nk
    inner = pl.ds(k0, nk)
    sides = {"py": (y, npy), "px": (x, npx), "pz": (z, npz)}

    def has(axis, side):
        index, count = sides[axis]
        return index > 0 if side == 0 else index < count - 1

    def beside(axis, side):
        return {axis: sides[axis][0] + (2 * side - 1)}

    def load_faces(m, side):
        return pltpu.make_async_copy(
            f_hbm.at[(nj - 1) * side, pl.ds(m * rows, rows)],
            fld.at[0, 1 + (nj - 1) * side, pl.ds(1 + m * rows, rows), inner],
            local.at[side, m],
        )

    def load_inner(m):
        return pltpu.make_async_copy(
            f_hbm.at[pl.ds(1, nj - 2), pl.ds(m * rows, rows)],
            fld.at[0, pl.ds(2, nj - 2), pl.ds(1 + m * rows, rows), inner],
            local.at[2, m],
        )

    def load_earlier(m):
        return pltpu.make_async_copy(
            e_hbm.at[:, pl.ds(m * rows, rows)],
            fld.at[1, pl.ds(1, nj), pl.ds(1 + m * rows, rows), inner],
            local.at[3, m],
        )

    def load_speed(m):
        return pltpu.make_async_copy(c_hbm.at[:, pl.ds(m * rows, rows)], csq.at[:, pl.ds(m * rows, rows)], local.at[4, m])

    def plane(p, m, side):
        span = pl.ds(1 + m * rows, rows)
        return pltpu.make_async_remote_copy(
            fld.at[p, 1 + (nj - 1) * side, span, inner],
            fld.at[p, (nj + 1) * (1 - side), span, inner],
            jsend.at[p, side, m], jrecv.at[p, 1 - side, m],
            device_id=beside("py", side), device_id_type=MESH,
        )

    def last_plane(q, h, side):
        span, tile = pl.ds(1 + h * long, long), pl.ds(k0 + q * TILE, TILE)
        return pltpu.make_async_remote_copy(
            fld.at[final, 1 + (nj - 1) * side, span, tile],
            fld.at[final, (nj + 1) * (1 - side), span, tile],
            lsend.at[side, q, h], lrecv.at[1 - side, q, h],
            device_id=beside("py", side), device_id_type=MESH,
        )

    def edge_k(p, m, side):
        span = pl.ds(1 + m * rows, rows)
        return pltpu.make_async_remote_copy(
            fld.at[p, pl.ds(1, nj), span, pl.ds((k1 - 1) if side else k0, 1)],
            fld.at[p, pl.ds(1, nj), span, pl.ds((k0 - 1) if side else k1, 1)],
            ksend.at[p, side, m], krecv.at[p, 1 - side, m],
            device_id=beside("pz", side), device_id_type=MESH,
        )

    def edge_i(p, side):
        return pltpu.make_async_remote_copy(
            fld.at[p, pl.ds(1, nj), ni if side else 1, inner],
            fld.at[p, pl.ds(1, nj), 0 if side else ni + 1, inner],
            isend.at[p, side], irecv.at[p, 1 - side],
            device_id=beside("px", side), device_id_type=MESH,
        )

    def wait_from(copy):
        copy.wait_recv()

    def each_side(axis, do):
        for side in (0, 1):
            pl.when(has(axis, side))(functools.partial(do, side))

    def over_chunks(do):
        def body(m, _):
            do(m)
            return 0
        lax.fori_loop(0, CHUNKS, body, 0)

    def start_loads(m):
        load_faces(m, 0).start()
        load_faces(m, 1).start()

    over_chunks(start_loads)

    def start_rest(m):
        load_inner(m).start()
        load_earlier(m).start()
        load_speed(m).start()

    over_chunks(start_rest)

    barrier = pltpu.get_barrier_semaphore()
    expected = jnp.int32(npx - 1)
    for axis in ("py", "pz"):
        for side in (0, 1):
            expected = expected + has(axis, side).astype(jnp.int32)

            @pl.when(has(axis, side))
            def _(axis=axis, side=side):
                pl.semaphore_signal(barrier, inc=1, device_id=beside(axis, side), device_id_type=MESH)

    for hop in range(1, npx):
        pl.semaphore_signal(barrier, inc=1, device_id={"px": lax.rem(x + hop, npx)}, device_id_type=MESH)
    pl.semaphore_wait(barrier, expected)

    def first_planes(m):
        load_faces(m, 0).wait()
        load_faces(m, 1).wait()
        each_side("py", lambda side: plane(0, m, side).start())

    over_chunks(first_planes)

    def first_edges(m):
        load_inner(m).wait()
        each_side("pz", lambda side: edge_k(0, m, side).start())

    over_chunks(first_edges)
    each_side("px", lambda side: edge_i(0, side).start())

    for side in (0, 1):
        @pl.when(jnp.logical_not(has("py", side)))
        def _(side=side):
            def clear(i, _):
                for p in (0, 1):
                    fld[p, (nj + 1) * side, i + 1, k0:k1] = jnp.zeros((nk, fld.shape[-1]), jnp.float32)
                return 0
            lax.fori_loop(0, ni, clear, 0)

        @pl.when(jnp.logical_not(has("px", side)))
        def _(side=side):
            for p in (0, 1):
                for j in range(nj):
                    fld[p, j + 1, (ni + 1) * side, k0:k1] = jnp.zeros((nk, fld.shape[-1]), jnp.float32)

        @pl.when(jnp.logical_not(has("pz", side)))
        def _(side=side):
            at = k1 if side else k0 - 8
            def clear(i, _):
                for p in (0, 1):
                    for j in range(nj):
                        fld[p, j + 1, i + 1, at:at + 8] = jnp.zeros((8, fld.shape[-1]), jnp.float32)
                return 0
            lax.fori_loop(0, ni, clear, 0)

    def advance(p, j, first, count, ks, put, shift=None, sums=None):
        lo, hi = k0 + ks[0], k0 + ks[1]

        def row(r, carry):
            before, middle = carry[:2]
            i = first + r + 1
            after = fld[p, j + 1, i + 1, lo:hi]
            along_j = fld[p, j, i, lo:hi] + fld[p, j + 2, i, lo:hi]
            along_k = fld[p, j + 1, i, lo - 1:hi - 1] + fld[p, j + 1, i, lo + 1:hi + 1]
            spread = (along_j + (before + after)) + along_k - 6.0 * middle
            later = 2.0 * middle - fld[1 - p, j + 1, i, lo:hi] + csq[j, i - 1, ks[0]:ks[1]] * spread
            put(i - 1, later)
            if sums is None:
                return middle, after
            moved = later - shift
            return middle, after, carry[2] + moved, carry[3] + moved * moved

        carry = (fld[p, j + 1, first, lo:hi], fld[p, j + 1, first + 1, lo:hi]) + (sums or ())
        return lax.fori_loop(0, count, row, carry, unroll=4)[2:]

    def with_edges(m, do):
        for side, at in ((0, 0), (1, CHUNKS - 1)):
            pl.when(jnp.logical_and(has("px", side), m == at))(functools.partial(do, side))

    for s in range(STEPS - 1):
        p, q = s % 2, 1 - s % 2

        def chunk(m, s=s, p=p, q=q):
            if s == 0:
                load_earlier(m).wait()
                load_speed(m).wait()
            each_side("pz", lambda side: edge_k(p, m, 1 - side).wait_recv())
            with_edges(m, lambda side: edge_i(p, 1 - side).wait_recv())
            if s > 0:
                each_side("py", lambda side: plane(q, m, side).wait_send())
                each_side("pz", lambda side: edge_k(q, m, side).wait_send())
                with_edges(m, lambda side: edge_i(q, side).wait_send())
            each_side("py", lambda side: plane(p, m, 1 - side).wait_recv())
            for j in range(nj):
                def put(i, later, j=j):
                    fld[q, j + 1, i + 1, k0:k1] = later

                advance(p, j, m * rows, rows, (0, nk), put)
            if s < STEPS - 2:
                each_side("py", lambda side: plane(q, m, side).start())
            else:
                per = CHUNKS // SPANS

                @pl.when(lax.rem(m, per) == per - 1)
                def _():
                    each_side("py", lambda side: last_plane(0, m // per, side).start())
            each_side("pz", lambda side: edge_k(q, m, side).start())
            with_edges(m, lambda side: edge_i(q, side).start())

        over_chunks(chunk)

    def over_spans(do):
        def body(h, _):
            do(h)
            return 0
        lax.fori_loop(0, SPANS, body, 0)

    for q in range(1, tiles):
        over_spans(lambda h, q=q: each_side("py", lambda side: last_plane(q, h, side).start()))

    p = final
    peers = [lax.rem(x + hop, npx) for hop in range(1, npx)]

    def share(buffer, group):
        return [
            pltpu.make_async_remote_copy(
                buffer.at[x], buffer.at[x], tsend.at[group, n], trecv.at[group, n],
                device_id={"px": peer}, device_id_type=MESH,
            )
            for n, peer in enumerate(peers)
        ]

    def local_sums(first, second, shift):
        mean = first * (1.0 / ni)
        return shift + mean, second - first * mean

    def line_sums(parts):
        mean = parts[0][0]
        for part in parts[1:]:
            mean = mean + part[0]
        mean = mean * (1.0 / npx)
        squares = jnp.zeros_like(mean)
        for part in parts:
            off = part[0] - mean
            squares = squares + (part[1] + ni * (off * off))
        return mean, lax.rsqrt(squares * (1.0 / (ni * npx)) + 0.0001)

    over_chunks(lambda m: each_side("pz", lambda side: edge_k(p, m, 1 - side).wait_recv()))
    each_side("px", lambda side: edge_i(p, 1 - side).wait_recv())
    for j in range(1, nj - 1):
        def put(i, later, j=j):
            out[j, i] = later

        shift = fld[p, j + 1, 1, k0:k1]
        zero = jnp.zeros_like(shift)
        sums = advance(p, j, 0, ni, (0, nk), put, shift, (zero, zero))
        inner_sums[x, 0, j - 1], inner_sums[x, 1, j - 1] = local_sums(*sums, shift)
    for copy in share(inner_sums, tiles):
        copy.start()

    def settle_inner():
        for copy in share(inner_sums, tiles):
            copy.wait()
        mean, scale = line_sums([(inner_sums[n, 0], inner_sums[n, 1]) for n in range(npx)])
        stat[0, 1:nj - 1] = mean
        stat[1, 1:nj - 1] = scale

    def settle_faces(q):
        for copy in share(face_sums.at[q], q):
            copy.wait()
        for f, j in enumerate((0, nj - 1)):
            mean, scale = line_sums([(face_sums[q, n, 0, f], face_sums[q, n, 1, f]) for n in range(npx)])
            stat[0, j, q * TILE:(q + 1) * TILE] = mean
            stat[1, j, q * TILE:(q + 1) * TILE] = scale

    for q in range(tiles):
        ks = (q * TILE, (q + 1) * TILE)
        shifts = [fld[p, j + 1, 1, k0 + ks[0]:k0 + ks[1]] for j in (0, nj - 1)]
        acc[...] = jnp.zeros_like(acc)

        def span(h, q=q, ks=ks, shifts=shifts):
            each_side("py", lambda side: last_plane(q, h, 1 - side).wait_recv())
            for f, j in enumerate((0, nj - 1)):
                def put(i, later, j=j):
                    out[j, i, ks[0]:ks[1]] = later

                acc[f, 0], acc[f, 1] = advance(p, j, h * long, long, ks, put, shifts[f], (acc[f, 0], acc[f, 1]))

        over_spans(span)
        for f in range(2):
            face_sums[q, x, 0, f], face_sums[q, x, 1, f] = local_sums(acc[f, 0], acc[f, 1], shifts[f])
        for copy in share(face_sums.at[q], q):
            copy.start()
        if q == 0:
            settle_inner()
        else:
            settle_faces(q - 1)

    for q in range(tiles):
        over_spans(lambda h, q=q: each_side("py", lambda side: last_plane(q, h, side).wait_send()))

    def finish(m):
        each_side("py", lambda side: plane(1 - p, m, side).wait_send())
        each_side("pz", lambda side: edge_k(1 - p, m, side).wait_send())
        each_side("pz", lambda side: edge_k(p, m, side).wait_send())

    over_chunks(finish)
    for t in (1 - p, p):
        each_side("px", lambda side: edge_i(t, side).wait_send())
    settle_faces(tiles - 1)


def normalise(f_ref, stat_ref, anomaly_hbm, end_hbm, staged, sems, end_sem):
    nj, ni = f_ref.shape[:2]
    rows = ni // CHUNKS
    ends = [pltpu.make_async_copy(f_ref.at[j], end_hbm.at[j], end_sem.at[j]) for j in range(nj)]
    for copy in ends:
        copy.start()

    def leave(m):
        return pltpu.make_async_copy(
            staged.at[:, pl.ds(m * rows, rows)], anomaly_hbm.at[:, pl.ds(m * rows, rows)], sems.at[m]
        )

    def chunk(m, _):
        for j in range(nj):
            mean, scale = stat_ref[0, j], stat_ref[1, j]

            def row(r, _):
                staged[j, m * rows + r] = (f_ref[j, m * rows + r] - mean) * scale
                return 0

            lax.fori_loop(0, rows, row, 0, unroll=4)
        leave(m).start()
        return 0

    lax.fori_loop(0, CHUNKS, chunk, 0)

    def done(m, _):
        leave(m).wait()
        return 0

    lax.fori_loop(0, CHUNKS, done, 0)
    for copy in ends:
        copy.wait()


def solution(mesh):
    npy, npx, npz = (mesh.shape[a] for a in ("py", "px", "pz"))

    def shards(field_now, earlier, speed_square):
        nj, ni, nk, nl = field_now.shape
        f32 = jnp.float32
        dma = pltpu.SemaphoreType.DMA
        hbm = pl.BlockSpec(memory_space=pltpu.HBM)
        vmem = pl.BlockSpec(memory_space=pltpu.VMEM)
        end, stat = pl.pallas_call(
            functools.partial(leapfrog, (nj, ni, nk, npy, npx, npz)),
            out_shape=(pltpu.VMEM((nj, ni, nk, nl), f32), pltpu.VMEM((2, nj, nk, nl), f32)),
            in_specs=[hbm] * 3,
            out_specs=(vmem, vmem),
            scratch_shapes=[
                pltpu.VMEM((2, nj + 2, ni + 2, nk + 2 * PAD, nl), f32),
                pltpu.VMEM((nj, ni, nk, nl), f32),
                pltpu.VMEM((2, 2, TILE, nl), f32),
                pltpu.VMEM((npx, 2, nj - 2, nk, nl), f32),
                pltpu.VMEM((nk // TILE, npx, 2, 2, TILE, nl), f32),
                dma((2, 2, CHUNKS)), dma((2, 2, CHUNKS)),
                dma((2, nk // TILE, SPANS)), dma((2, nk // TILE, SPANS)),
                dma((2, 2, CHUNKS)), dma((2, 2, CHUNKS)),
                dma((2, 2)), dma((2, 2)),
                dma((nk // TILE + 1, npx - 1)), dma((nk // TILE + 1, npx - 1)),
                dma((5, CHUNKS)),
            ],
            compiler_params=pltpu.CompilerParams(
                collective_id=0, has_side_effects=True, vmem_limit_bytes=48 << 20
            ),
            name="leapfrog",
        )(field_now, earlier, speed_square)
        return pl.pallas_call(
            normalise,
            out_shape=(jax.ShapeDtypeStruct((nj, ni, nk, nl), f32),) * 2,
            in_specs=[vmem, vmem],
            out_specs=(hbm, hbm),
            scratch_shapes=[pltpu.VMEM((nj, ni, nk, nl), f32), dma((CHUNKS,)), dma((nj,))],
            compiler_params=pltpu.CompilerParams(vmem_limit_bytes=20 << 20),
            name="normalise",
        )(end, stat)

    spec = P("py", "px", "pz", None)
    return jax.shard_map(shards, mesh=mesh, in_specs=(spec,) * 3, out_specs=(spec,) * 2, check_vma=False)
```

```python
import functools

import jax
import jax.numpy as jnp
from jax import lax
from jax.experimental import pallas as pl
from jax.experimental.pallas import tpu as pltpu
from jax.sharding import PartitionSpec as P

STEPS = 4
CHUNKS = 4
SPANS = 4
TILE = 8
PARTS = 8
MESH = pl.DeviceIdType.MESH
PAD = 8


def leapfrog(dims, f_hbm, e_hbm, c_hbm, out, stat, fld, csq, acc, inner_sums, face_sums, jsend, jrecv, lsend, lrecv, ksend, krecv, isend, irecv, tsend, trecv, local):
    nj, ni, nk, npy, npx, npz = dims
    rows, long = ni // CHUNKS, ni // SPANS
    tiles = nk // TILE
    final = (STEPS - 1) % 2
    y, x, z = lax.axis_index("py"), lax.axis_index("px"), lax.axis_index("pz")
    k0, k1 = PAD, PAD + nk
    inner = pl.ds(k0, nk)
    everything = pl.ds(1, ni)
    sides = {"py": (y, npy), "px": (x, npx), "pz": (z, npz)}

    def has(axis, side):
        index, count = sides[axis]
        return index > 0 if side == 0 else index < count - 1

    def beside(axis, side):
        return {axis: sides[axis][0] + (2 * side - 1)}

    def span_of(m):
        return pl.ds(1 + m * rows, rows)

    def load_faces(side, part):
        start, size = ((0, rows), (rows, ni - rows))[part]
        return pltpu.make_async_copy(
            f_hbm.at[(nj - 1) * side, pl.ds(start, size)],
            fld.at[0, 1 + (nj - 1) * side, pl.ds(1 + start, size), inner],
            local.at[2 * part + side],
        )

    def load_inner():
        return pltpu.make_async_copy(
            f_hbm.at[pl.ds(1, nj - 2)], fld.at[0, pl.ds(2, nj - 2), everything, inner], local.at[4]
        )

    def load_earlier():
        return pltpu.make_async_copy(e_hbm, fld.at[1, pl.ds(1, nj), everything, inner], local.at[5])

    def load_speed():
        return pltpu.make_async_copy(c_hbm, csq, local.at[6])

    def face_copy(p, span, tile, side, sent, received):
        return pltpu.make_async_remote_copy(
            fld.at[p, 1 + (nj - 1) * side, span, tile],
            fld.at[p, (nj + 1) * (1 - side), span, tile],
            sent, received, device_id=beside("py", side), device_id_type=MESH,
        )

    def plane(p, m, side):
        return face_copy(p, span_of(m), inner, side, jsend.at[p, side], jrecv.at[p, 1 - side, m])

    def sent_planes(p, side):
        return face_copy(p, everything, inner, side, jsend.at[p, side], jrecv.at[p, 1 - side, 0])

    def last_plane(q, h, side):
        span = everything if h is None else pl.ds(1 + h * long, long)
        slot = tiles - 1 + h if q == tiles - 1 else q
        return face_copy(final, span, pl.ds(k0 + q * TILE, TILE), side, lsend.at[side], lrecv.at[1 - side, slot])

    def sent_last(side):
        return face_copy(final, everything, inner, side, lsend.at[side], lrecv.at[1 - side, 0])

    def edge_k(p, m, side):
        span = everything if m is None else span_of(m)
        return pltpu.make_async_remote_copy(
            fld.at[p, pl.ds(1, nj), span, pl.ds((k1 - 1) if side else k0, 1)],
            fld.at[p, pl.ds(1, nj), span, pl.ds((k0 - 1) if side else k1, 1)],
            ksend.at[p, side], krecv.at[p, 1 - side],
            device_id=beside("pz", side), device_id_type=MESH,
        )

    def edge_i(p, side):
        return pltpu.make_async_remote_copy(
            fld.at[p, pl.ds(1, nj), ni if side else 1, inner],
            fld.at[p, pl.ds(1, nj), 0 if side else ni + 1, inner],
            isend.at[p, side], irecv.at[p, 1 - side],
            device_id=beside("px", side), device_id_type=MESH,
        )

    def each_side(axis, do):
        for side in (0, 1):
            pl.when(has(axis, side))(functools.partial(do, side))

    def repeat(count, do, start=0):
        def body(m, _):
            do(m)
            return 0
        lax.fori_loop(start, count, body, 0)

    for part in (0, 1):
        for side in (0, 1):
            load_faces(side, part).start()

    barrier = pltpu.get_barrier_semaphore()
    expected = jnp.int32(0)
    for axis in ("py", "px", "pz"):
        for side in (0, 1):
            expected = expected + has(axis, side).astype(jnp.int32)

            @pl.when(has(axis, side))
            def _(axis=axis, side=side):
                pl.semaphore_signal(barrier, inc=1, device_id=beside(axis, side), device_id_type=MESH)

    pl.semaphore_wait(barrier, expected)

    for part, (start, stop) in enumerate(((0, 1), (1, CHUNKS))):
        for side in (0, 1):
            load_faces(side, part).wait()
        repeat(stop, lambda m: each_side("py", lambda side: plane(0, m, side).start()), start)

    load_inner().start()
    load_earlier().start()
    load_speed().start()
    load_inner().wait()
    each_side("pz", lambda side: edge_k(0, None, side).start())
    each_side("px", lambda side: edge_i(0, side).start())

    for side in (0, 1):
        @pl.when(jnp.logical_not(has("py", side)))
        def _(side=side):
            def clear(i):
                for p in (0, 1):
                    fld[p, (nj + 1) * side, i + 1, k0:k1] = jnp.zeros((nk, fld.shape[-1]), jnp.float32)
            repeat(ni, clear)

        @pl.when(jnp.logical_not(has("px", side)))
        def _(side=side):
            for p in (0, 1):
                for j in range(nj):
                    fld[p, j + 1, (ni + 1) * side, k0:k1] = jnp.zeros((nk, fld.shape[-1]), jnp.float32)

        @pl.when(jnp.logical_not(has("pz", side)))
        def _(side=side):
            at = k1 if side else k0 - 8
            def clear(i):
                for p in (0, 1):
                    for j in range(nj):
                        fld[p, j + 1, i + 1, at:at + 8] = jnp.zeros((8, fld.shape[-1]), jnp.float32)
            repeat(ni, clear)

    def advance(p, j, first, count, ks, put, shift=None, sums=None):
        lo, hi = k0 + ks[0], k0 + ks[1]

        def row(r, carry):
            before, middle = carry[:2]
            i = first + r + 1
            after = fld[p, j + 1, i + 1, lo:hi]
            along_j = fld[p, j, i, lo:hi] + fld[p, j + 2, i, lo:hi]
            along_k = fld[p, j + 1, i, lo - 1:hi - 1] + fld[p, j + 1, i, lo + 1:hi + 1]
            spread = (along_j + (before + after)) + along_k - 6.0 * middle
            later = 2.0 * middle - fld[1 - p, j + 1, i, lo:hi] + csq[j, i - 1, ks[0]:ks[1]] * spread
            put(i - 1, later)
            if sums is None:
                return middle, after
            moved = later - shift
            return middle, after, carry[2] + moved, carry[3] + moved * moved

        carry = (fld[p, j + 1, first, lo:hi], fld[p, j + 1, first + 1, lo:hi]) + (sums or ())
        return lax.fori_loop(0, count, row, carry, unroll=4)[2:]

    def with_edges(m, do):
        for side, at in ((0, 0), (1, CHUNKS - 1)):
            pl.when(jnp.logical_and(has("px", side), m == at))(functools.partial(do, side))

    for s in range(STEPS - 1):
        p, q = s % 2, 1 - s % 2
        if s == 0:
            load_earlier().wait()
            load_speed().wait()
        else:
            each_side("py", lambda side: sent_planes(q, side).wait_send())
            each_side("pz", lambda side: edge_k(q, None, side).wait_send())
            each_side("px", lambda side: edge_i(q, side).wait_send())
        each_side("pz", lambda side: edge_k(p, None, 1 - side).wait_recv())
        each_side("px", lambda side: edge_i(p, 1 - side).wait_recv())

        def chunk(m, s=s, p=p, q=q):
            each_side("py", lambda side: plane(p, m, 1 - side).wait_recv())
            for j in range(nj):
                def put(i, later, j=j):
                    fld[q, j + 1, i + 1, k0:k1] = later

                advance(p, j, m * rows, rows, (0, nk), put)
            if s < STEPS - 2:
                each_side("py", lambda side: plane(q, m, side).start())
            else:
                per = CHUNKS // SPANS

                @pl.when(lax.rem(m, per) == per - 1)
                def _():
                    each_side("py", lambda side: last_plane(0, m // per, side).start())
            each_side("pz", lambda side: edge_k(q, m, side).start())
            with_edges(m, lambda side: edge_i(q, side).start())

        repeat(CHUNKS, chunk)

    for q in range(1, tiles - 1):
        each_side("py", lambda side: last_plane(q, None, side).start())
    repeat(SPANS, lambda h: each_side("py", lambda side: last_plane(tiles - 1, h, side).start()))

    p = final
    peers = [lax.rem(x + hop, npx) for hop in range(1, npx)]

    def share(buffer, group):
        for peer in peers:
            pltpu.make_async_remote_copy(
                buffer.at[x], buffer.at[x], tsend.at[group // tiles], trecv.at[group],
                device_id={"px": peer}, device_id_type=MESH,
            ).start()

    def shared(cells, group):
        return pltpu.make_async_remote_copy(
            cells, cells, tsend.at[group // tiles], trecv.at[group], device_id={"px": peers[0]}, device_id_type=MESH
        )

    others = pl.ds(0, npx - 1)

    def local_sums(first, second, shift):
        mean = first * (1.0 / ni)
        return shift + mean, second - first * mean

    def line_sums(parts):
        mean = parts[0][0]
        for part in parts[1:]:
            mean = mean + part[0]
        mean = mean * (1.0 / npx)
        squares = jnp.zeros_like(mean)
        for part in parts:
            off = part[0] - mean
            squares = squares + (part[1] + ni * (off * off))
        return mean, lax.rsqrt(squares * (1.0 / (ni * npx)) + 0.0001)

    each_side("pz", lambda side: edge_k(p, None, 1 - side).wait_recv())
    each_side("px", lambda side: edge_i(p, 1 - side).wait_recv())
    for j in range(1, nj - 1):
        def put(i, later, j=j):
            out[j, i] = later

        shift = fld[p, j + 1, 1, k0:k1]
        zero = jnp.zeros_like(shift)
        sums = advance(p, j, 0, ni, (0, nk), put, shift, (zero, zero))
        inner_sums[x, 0, j - 1], inner_sums[x, 1, j - 1] = local_sums(*sums, shift)
    share(inner_sums, tiles)

    def settle_inner():
        shared(inner_sums.at[others], tiles).wait_recv()
        mean, scale = line_sums([(inner_sums[n, 0], inner_sums[n, 1]) for n in range(npx)])
        stat[0, 1:nj - 1] = mean
        stat[1, 1:nj - 1] = scale

    def settle_faces(q):
        shared(face_sums.at[q, others], q).wait_recv()
        for f, j in enumerate((0, nj - 1)):
            mean, scale = line_sums([(face_sums[q, n, 0, f], face_sums[q, n, 1, f]) for n in range(npx)])
            stat[0, j, q * TILE:(q + 1) * TILE] = mean
            stat[1, j, q * TILE:(q + 1) * TILE] = scale

    for q in range(tiles):
        ks = (q * TILE, (q + 1) * TILE)
        shifts = [fld[p, j + 1, 1, k0 + ks[0]:k0 + ks[1]] for j in (0, nj - 1)]
        acc[...] = jnp.zeros_like(acc)

        pieces = SPANS if q == tiles - 1 else 1
        count = ni // pieces

        def span(h, q=q, ks=ks, shifts=shifts, pieces=pieces, count=count):
            each_side("py", lambda side: last_plane(q, h if pieces > 1 else None, 1 - side).wait_recv())
            for f, j in enumerate((0, nj - 1)):
                def put(i, later, j=j):
                    out[j, i, ks[0]:ks[1]] = later

                acc[f, 0], acc[f, 1] = advance(p, j, h * count, count, ks, put, shifts[f], (acc[f, 0], acc[f, 1]))

        repeat(pieces, span)
        for f in range(2):
            face_sums[q, x, 0, f], face_sums[q, x, 1, f] = local_sums(acc[f, 0], acc[f, 1], shifts[f])
        share(face_sums.at[q], q)
        if q == 0:
            settle_inner()
        else:
            settle_faces(q - 1)

    each_side("py", lambda side: sent_last(side).wait_send())
    each_side("py", lambda side: sent_planes(1 - p, side).wait_send())
    for t in (1 - p, p):
        each_side("pz", lambda side: edge_k(t, None, side).wait_send())
        each_side("px", lambda side: edge_i(t, side).wait_send())
    shared(inner_sums.at[others], tiles).wait_send()
    settle_faces(tiles - 1)
    shared(face_sums.at[:, others], 0).wait_send()


def normalise(f_ref, stat_ref, anomaly_hbm, end_hbm, staged, sems):
    nj, ni = f_ref.shape[:2]
    rows = ni // PARTS
    end = pltpu.make_async_copy(f_ref, end_hbm, sems.at[0])
    end.start()

    def chunk(m, _):
        for j in range(nj):
            mean, scale = stat_ref[0, j], stat_ref[1, j]

            def row(r, _):
                staged[j, m * rows + r] = (f_ref[j, m * rows + r] - mean) * scale
                return 0

            lax.fori_loop(0, rows, row, 0, unroll=4)
        piece = pl.ds(m * rows, rows)
        pltpu.make_async_copy(staged.at[:, piece], anomaly_hbm.at[:, piece], sems.at[1]).start()
        return 0

    lax.fori_loop(0, PARTS, chunk, 0)
    end.wait()
    pltpu.make_async_copy(staged, anomaly_hbm, sems.at[1]).wait()


def solution(mesh):
    npy, npx, npz = (mesh.shape[a] for a in ("py", "px", "pz"))

    def shards(field_now, earlier, speed_square):
        nj, ni, nk, nl = field_now.shape
        f32 = jnp.float32
        dma = pltpu.SemaphoreType.DMA
        hbm = pl.BlockSpec(memory_space=pltpu.HBM)
        vmem = pl.BlockSpec(memory_space=pltpu.VMEM)
        end, stat = pl.pallas_call(
            functools.partial(leapfrog, (nj, ni, nk, npy, npx, npz)),
            out_shape=(pltpu.VMEM((nj, ni, nk, nl), f32), pltpu.VMEM((2, nj, nk, nl), f32)),
            in_specs=[hbm] * 3,
            out_specs=(vmem, vmem),
            scratch_shapes=[
                pltpu.VMEM((2, nj + 2, ni + 2, nk + 2 * PAD, nl), f32),
                pltpu.VMEM((nj, ni, nk, nl), f32),
                pltpu.VMEM((2, 2, TILE, nl), f32),
                pltpu.VMEM((npx, 2, nj - 2, nk, nl), f32),
                pltpu.VMEM((nk // TILE, npx, 2, 2, TILE, nl), f32),
                dma((2, 2)), dma((2, 2, CHUNKS)),
                dma((2,)), dma((2, nk // TILE - 1 + SPANS)),
                dma((2, 2)), dma((2, 2)),
                dma((2, 2)), dma((2, 2)),
                dma((2,)), dma((nk // TILE + 1,)),
                dma((7,)),
            ],
            compiler_params=pltpu.CompilerParams(
                collective_id=0, has_side_effects=True, vmem_limit_bytes=48 << 20
            ),
            name="leapfrog",
        )(field_now, earlier, speed_square)
        return pl.pallas_call(
            normalise,
            out_shape=(jax.ShapeDtypeStruct((nj, ni, nk, nl), f32),) * 2,
            in_specs=[vmem, vmem],
            out_specs=(hbm, hbm),
            scratch_shapes=[pltpu.VMEM((nj, ni, nk, nl), f32), dma((2,))],
            compiler_params=pltpu.CompilerParams(vmem_limit_bytes=20 << 20),
            name="normalise",
        )(end, stat)

    spec = P("py", "px", "pz", None)
    return jax.shard_map(shards, mesh=mesh, in_specs=(spec,) * 3, out_specs=(spec,) * 2, check_vma=False)
```

```python
import functools

import jax
import jax.numpy as jnp
from jax import lax
from jax.experimental import pallas as pl
from jax.experimental.pallas import tpu as pltpu
from jax.sharding import PartitionSpec as P

STEPS = 4
CHUNKS = 4
SPANS = 4
TILE = 8
PARTS = 8
MESH = pl.DeviceIdType.MESH
PAD = 8


def leapfrog(dims, f_hbm, e_hbm, c_hbm, out, stat, fld, csq, acc, inner_sums, face_sums, jsend, jrecv, lsend, lrecv, ksend, krecv, isend, irecv, tsend, trecv, local):
    nj, ni, nk, npy, npx, npz = dims
    rows, long = ni // CHUNKS, ni // SPANS
    tiles = nk // TILE
    final = (STEPS - 1) % 2
    y, x, z = lax.axis_index("py"), lax.axis_index("px"), lax.axis_index("pz")
    k0, k1 = PAD, PAD + nk
    inner = pl.ds(k0, nk)
    everything = pl.ds(1, ni)
    sides = {"py": (y, npy), "px": (x, npx), "pz": (z, npz)}

    def has(axis, side):
        index, count = sides[axis]
        return index > 0 if side == 0 else index < count - 1

    def beside(axis, side):
        return {axis: sides[axis][0] + (2 * side - 1)}

    def span_of(m):
        return pl.ds(1 + m * rows, rows)

    def load_faces(side, part):
        start, size = ((0, rows), (rows, ni - rows))[part]
        return pltpu.make_async_copy(
            f_hbm.at[(nj - 1) * side, pl.ds(start, size)],
            fld.at[0, 1 + (nj - 1) * side, pl.ds(1 + start, size), inner],
            local.at[2 * part + side],
        )

    def load_inner():
        return pltpu.make_async_copy(
            f_hbm.at[pl.ds(1, nj - 2)], fld.at[0, pl.ds(2, nj - 2), everything, inner], local.at[4]
        )

    def load_earlier():
        return pltpu.make_async_copy(e_hbm, fld.at[1, pl.ds(1, nj), everything, inner], local.at[5])

    def load_speed():
        return pltpu.make_async_copy(c_hbm, csq, local.at[6])

    def face_copy(p, span, tile, side, sent, received):
        return pltpu.make_async_remote_copy(
            fld.at[p, 1 + (nj - 1) * side, span, tile],
            fld.at[p, (nj + 1) * (1 - side), span, tile],
            sent, received, device_id=beside("py", side), device_id_type=MESH,
        )

    def plane(p, m, side):
        return face_copy(p, span_of(m), inner, side, jsend.at[p, side], jrecv.at[p, 1 - side, m])

    def sent_planes(p, side):
        return face_copy(p, everything, inner, side, jsend.at[p, side], jrecv.at[p, 1 - side, 0])

    def last_plane(q, h, side):
        span = everything if h is None else pl.ds(1 + h * long, long)
        slot = tiles - 1 + h if q == tiles - 1 else q
        return face_copy(final, span, pl.ds(k0 + q * TILE, TILE), side, lsend.at[side], lrecv.at[1 - side, slot])

    def sent_last(side):
        return face_copy(final, everything, inner, side, lsend.at[side], lrecv.at[1 - side, 0])

    def edge_k(p, m, side):
        span = everything if m is None else span_of(m)
        return pltpu.make_async_remote_copy(
            fld.at[p, pl.ds(1, nj), span, pl.ds((k1 - 1) if side else k0, 1)],
            fld.at[p, pl.ds(1, nj), span, pl.ds((k0 - 1) if side else k1, 1)],
            ksend.at[p, side], krecv.at[p, 1 - side],
            device_id=beside("pz", side), device_id_type=MESH,
        )

    def edge_i(p, side):
        return pltpu.make_async_remote_copy(
            fld.at[p, pl.ds(1, nj), ni if side else 1, inner],
            fld.at[p, pl.ds(1, nj), 0 if side else ni + 1, inner],
            isend.at[p, side], irecv.at[p, 1 - side],
            device_id=beside("px", side), device_id_type=MESH,
        )

    def each_side(axis, do):
        for side in (0, 1):
            pl.when(has(axis, side))(functools.partial(do, side))

    def repeat(count, do, start=0):
        def body(m, _):
            do(m)
            return 0
        lax.fori_loop(start, count, body, 0)

    for part in (0, 1):
        for side in (0, 1):
            load_faces(side, part).start()

    barrier = pltpu.get_barrier_semaphore()
    expected = jnp.int32(0)
    for axis in ("py", "px", "pz"):
        for side in (0, 1):
            expected = expected + has(axis, side).astype(jnp.int32)

            @pl.when(has(axis, side))
            def _(axis=axis, side=side):
                pl.semaphore_signal(barrier, inc=1, device_id=beside(axis, side), device_id_type=MESH)

    pl.semaphore_wait(barrier, expected)

    for part, (start, stop) in enumerate(((0, 1), (1, CHUNKS))):
        for side in (0, 1):
            load_faces(side, part).wait()
        repeat(stop, lambda m: each_side("py", lambda side: plane(0, m, side).start()), start)

    load_inner().start()
    load_earlier().start()
    load_speed().start()
    load_inner().wait()
    each_side("pz", lambda side: edge_k(0, None, side).start())
    each_side("px", lambda side: edge_i(0, side).start())

    for side in (0, 1):
        @pl.when(jnp.logical_not(has("py", side)))
        def _(side=side):
            def clear(i):
                for p in (0, 1):
                    fld[p, (nj + 1) * side, i + 1, k0:k1] = jnp.zeros((nk, fld.shape[-1]), jnp.float32)
            repeat(ni, clear)

        @pl.when(jnp.logical_not(has("px", side)))
        def _(side=side):
            for p in (0, 1):
                for j in range(nj):
                    fld[p, j + 1, (ni + 1) * side, k0:k1] = jnp.zeros((nk, fld.shape[-1]), jnp.float32)

        @pl.when(jnp.logical_not(has("pz", side)))
        def _(side=side):
            at = k1 if side else k0 - 8
            def clear(i):
                for p in (0, 1):
                    for j in range(nj):
                        fld[p, j + 1, i + 1, at:at + 8] = jnp.zeros((8, fld.shape[-1]), jnp.float32)
            repeat(ni, clear)

    def later_at(p, j, i, before, middle, after, ks):
        lo, hi = k0 + ks[0], k0 + ks[1]
        along_j = fld[p, j, i, lo:hi] + fld[p, j + 2, i, lo:hi]
        along_k = fld[p, j + 1, i, lo - 1:hi - 1] + fld[p, j + 1, i, lo + 1:hi + 1]
        spread = (along_j + (before + after)) + along_k - 6.0 * middle
        return 2.0 * middle - fld[1 - p, j + 1, i, lo:hi] + csq[j, i - 1, ks[0]:ks[1]] * spread

    def sample(p, j, ks):
        i, cells = long // 2 + 1, slice(k0 + ks[0], k0 + ks[1])
        return later_at(p, j, i, fld[p, j + 1, i - 1, cells], fld[p, j + 1, i, cells], fld[p, j + 1, i + 1, cells], ks)

    def advance(p, j, first, count, ks, put, shift=None, sums=None):
        lo, hi = k0 + ks[0], k0 + ks[1]

        def row(r, carry):
            before, middle = carry[:2]
            i = first + r + 1
            after = fld[p, j + 1, i + 1, lo:hi]
            later = later_at(p, j, i, before, middle, after, ks)
            put(i - 1, later)
            if sums is None:
                return middle, after
            moved = later - shift
            return middle, after, carry[2] + moved, carry[3] + moved * moved

        carry = (fld[p, j + 1, first, lo:hi], fld[p, j + 1, first + 1, lo:hi]) + (sums or ())
        return lax.fori_loop(0, count, row, carry, unroll=4)[2:]

    def with_edges(m, do):
        for side, at in ((0, 0), (1, CHUNKS - 1)):
            pl.when(jnp.logical_and(has("px", side), m == at))(functools.partial(do, side))

    for s in range(STEPS - 1):
        p, q = s % 2, 1 - s % 2
        if s == 0:
            load_earlier().wait()
            load_speed().wait()
        else:
            each_side("py", lambda side: sent_planes(q, side).wait_send())
            each_side("pz", lambda side: edge_k(q, None, side).wait_send())
            each_side("px", lambda side: edge_i(q, side).wait_send())
        each_side("pz", lambda side: edge_k(p, None, 1 - side).wait_recv())
        each_side("px", lambda side: edge_i(p, 1 - side).wait_recv())

        def chunk(m, s=s, p=p, q=q):
            each_side("py", lambda side: plane(p, m, 1 - side).wait_recv())
            for j in range(nj):
                def put(i, later, j=j):
                    fld[q, j + 1, i + 1, k0:k1] = later

                advance(p, j, m * rows, rows, (0, nk), put)
            if s < STEPS - 2:
                each_side("py", lambda side: plane(q, m, side).start())
            else:
                per = CHUNKS // SPANS

                @pl.when(lax.rem(m, per) == per - 1)
                def _():
                    each_side("py", lambda side: last_plane(0, m // per, side).start())
            each_side("pz", lambda side: edge_k(q, m, side).start())
            with_edges(m, lambda side: edge_i(q, side).start())

        repeat(CHUNKS, chunk)

    for q in range(1, tiles - 1):
        each_side("py", lambda side: last_plane(q, None, side).start())
    repeat(SPANS, lambda h: each_side("py", lambda side: last_plane(tiles - 1, h, side).start()))

    p = final
    peers = [lax.rem(x + hop, npx) for hop in range(1, npx)]

    def share(buffer, group):
        for peer in peers:
            pltpu.make_async_remote_copy(
                buffer.at[x], buffer.at[x], tsend.at[group // tiles], trecv.at[group],
                device_id={"px": peer}, device_id_type=MESH,
            ).start()

    def shared(cells, group):
        return pltpu.make_async_remote_copy(
            cells, cells, tsend.at[group // tiles], trecv.at[group], device_id={"px": peers[0]}, device_id_type=MESH
        )

    others = pl.ds(0, npx - 1)

    def local_sums(first, second, shift):
        mean = first * (1.0 / ni)
        return shift + mean, second - first * mean

    def line_sums(parts):
        mean = parts[0][0]
        for part in parts[1:]:
            mean = mean + part[0]
        mean = mean * (1.0 / npx)
        squares = jnp.zeros_like(mean)
        for part in parts:
            off = part[0] - mean
            squares = squares + (part[1] + ni * (off * off))
        return mean, lax.rsqrt(squares * (1.0 / (ni * npx)) + 0.0001)

    each_side("pz", lambda side: edge_k(p, None, 1 - side).wait_recv())
    each_side("px", lambda side: edge_i(p, 1 - side).wait_recv())
    for j in range(1, nj - 1):
        def put(i, later, j=j):
            out[j, i] = later

        shift = sample(p, j, (0, nk))
        zero = jnp.zeros_like(shift)
        sums = advance(p, j, 0, ni, (0, nk), put, shift, (zero, zero))
        inner_sums[x, 0, j - 1], inner_sums[x, 1, j - 1] = local_sums(*sums, shift)
    share(inner_sums, tiles)

    def settle_inner():
        shared(inner_sums.at[others], tiles).wait_recv()
        mean, scale = line_sums([(inner_sums[n, 0], inner_sums[n, 1]) for n in range(npx)])
        stat[0, 1:nj - 1] = mean
        stat[1, 1:nj - 1] = scale

    def settle_faces(q):
        shared(face_sums.at[q, others], q).wait_recv()
        for f, j in enumerate((0, nj - 1)):
            mean, scale = line_sums([(face_sums[q, n, 0, f], face_sums[q, n, 1, f]) for n in range(npx)])
            stat[0, j, q * TILE:(q + 1) * TILE] = mean
            stat[1, j, q * TILE:(q + 1) * TILE] = scale

    for q in range(tiles):
        ks = (q * TILE, (q + 1) * TILE)
        pieces = SPANS if q == tiles - 1 else 1
        count = ni // pieces

        def span(h, q=q, ks=ks, pieces=pieces, count=count):
            each_side("py", lambda side: last_plane(q, h if pieces > 1 else None, 1 - side).wait_recv())

            @pl.when(h == 0)
            def _():
                for f, j in enumerate((0, nj - 1)):
                    acc[f, 0] = jnp.zeros(acc.shape[2:], jnp.float32)
                    acc[f, 1] = jnp.zeros(acc.shape[2:], jnp.float32)
                    acc[f, 2] = sample(p, j, ks)

            for f, j in enumerate((0, nj - 1)):
                def put(i, later, j=j):
                    out[j, i, ks[0]:ks[1]] = later

                sums = advance(p, j, h * count, count, ks, put, acc[f, 2], (acc[f, 0], acc[f, 1]))
                acc[f, 0], acc[f, 1] = sums

        repeat(pieces, span)
        for f in range(2):
            face_sums[q, x, 0, f], face_sums[q, x, 1, f] = local_sums(acc[f, 0], acc[f, 1], acc[f, 2])
        share(face_sums.at[q], q)
        if q == 0:
            settle_inner()
        else:
            settle_faces(q - 1)

    each_side("py", lambda side: sent_last(side).wait_send())
    each_side("py", lambda side: sent_planes(1 - p, side).wait_send())
    for t in (1 - p, p):
        each_side("pz", lambda side: edge_k(t, None, side).wait_send())
        each_side("px", lambda side: edge_i(t, side).wait_send())
    shared(inner_sums.at[others], tiles).wait_send()
    settle_faces(tiles - 1)
    shared(face_sums.at[:, others], 0).wait_send()


def normalise(f_ref, stat_ref, anomaly_hbm, end_hbm, staged, sems):
    nj, ni = f_ref.shape[:2]
    rows = ni // PARTS
    end = pltpu.make_async_copy(f_ref, end_hbm, sems.at[0])
    for j in range(nj):
        for m in range(8):
            piece = pl.ds(m * (ni // 8), ni // 8)
            pltpu.make_async_copy(f_ref.at[j, piece], end_hbm.at[j, piece], sems.at[0]).start()

    def chunk(m, _):
        for j in range(nj):
            mean, scale = stat_ref[0, j], stat_ref[1, j]

            def row(r, _):
                staged[j, m * rows + r] = (f_ref[j, m * rows + r] - mean) * scale
                return 0

            lax.fori_loop(0, rows, row, 0, unroll=4)
        piece = pl.ds(m * rows, rows)
        pltpu.make_async_copy(staged.at[:, piece], anomaly_hbm.at[:, piece], sems.at[1]).start()
        return 0

    lax.fori_loop(0, PARTS, chunk, 0)
    end.wait()
    pltpu.make_async_copy(staged, anomaly_hbm, sems.at[1]).wait()


def solution(mesh):
    npy, npx, npz = (mesh.shape[a] for a in ("py", "px", "pz"))

    def shards(field_now, earlier, speed_square):
        nj, ni, nk, nl = field_now.shape
        f32 = jnp.float32
        dma = pltpu.SemaphoreType.DMA
        hbm = pl.BlockSpec(memory_space=pltpu.HBM)
        vmem = pl.BlockSpec(memory_space=pltpu.VMEM)
        end, stat = pl.pallas_call(
            functools.partial(leapfrog, (nj, ni, nk, npy, npx, npz)),
            out_shape=(pltpu.VMEM((nj, ni, nk, nl), f32), pltpu.VMEM((2, nj, nk, nl), f32)),
            in_specs=[hbm] * 3,
            out_specs=(vmem, vmem),
            scratch_shapes=[
                pltpu.VMEM((2, nj + 2, ni + 2, nk + 2 * PAD, nl), f32),
                pltpu.VMEM((nj, ni, nk, nl), f32),
                pltpu.VMEM((2, 3, TILE, nl), f32),
                pltpu.VMEM((npx, 2, nj - 2, nk, nl), f32),
                pltpu.VMEM((nk // TILE, npx, 2, 2, TILE, nl), f32),
                dma((2, 2)), dma((2, 2, CHUNKS)),
                dma((2,)), dma((2, nk // TILE - 1 + SPANS)),
                dma((2, 2)), dma((2, 2)),
                dma((2, 2)), dma((2, 2)),
                dma((2,)), dma((nk // TILE + 1,)),
                dma((7,)),
            ],
            compiler_params=pltpu.CompilerParams(
                collective_id=0, has_side_effects=True, vmem_limit_bytes=48 << 20
            ),
            name="leapfrog",
        )(field_now, earlier, speed_square)
        return pl.pallas_call(
            normalise,
            out_shape=(jax.ShapeDtypeStruct((nj, ni, nk, nl), f32),) * 2,
            in_specs=[vmem, vmem],
            out_specs=(hbm, hbm),
            scratch_shapes=[pltpu.VMEM((nj, ni, nk, nl), f32), dma((2,))],
            compiler_params=pltpu.CompilerParams(vmem_limit_bytes=20 << 20),
            name="normalise",
        )(end, stat)

    spec = P("py", "px", "pz", None)
    return jax.shard_map(shards, mesh=mesh, in_specs=(spec,) * 3, out_specs=(spec,) * 2, check_vma=False)
```

```python
import functools

import jax
import jax.numpy as jnp
from jax import lax
from jax.experimental import pallas as pl
from jax.experimental.pallas import tpu as pltpu
from jax.sharding import PartitionSpec as P

STEPS = 4
CHUNKS = 4
SPANS = 4
TILE = 8
PARTS = 8
MESH = pl.DeviceIdType.MESH
PAD = 8


def leapfrog(dims, f_hbm, e_hbm, c_hbm, out, stat, fld, csq, acc, inner_sums, face_sums, jsend, jrecv, lsend, lrecv, ksend, krecv, isend, irecv, tsend, trecv, local):
    nj, ni, nk, npy, npx, npz = dims
    rows, long = ni // CHUNKS, ni // SPANS
    tiles = nk // TILE
    final = (STEPS - 1) % 2
    y, x, z = lax.axis_index("py"), lax.axis_index("px"), lax.axis_index("pz")
    k0, k1 = PAD, PAD + nk
    inner = pl.ds(k0, nk)
    everything = pl.ds(1, ni)
    sides = {"py": (y, npy), "px": (x, npx), "pz": (z, npz)}

    def has(axis, side):
        index, count = sides[axis]
        return index > 0 if side == 0 else index < count - 1

    def beside(axis, side):
        return {axis: sides[axis][0] + (2 * side - 1)}

    def span_of(m):
        return pl.ds(1 + m * rows, rows)

    def load_faces(side, part):
        start, size = ((0, rows), (rows, ni - rows))[part]
        return pltpu.make_async_copy(
            f_hbm.at[(nj - 1) * side, pl.ds(start, size)],
            fld.at[0, 1 + (nj - 1) * side, pl.ds(1 + start, size), inner],
            local.at[2 * part + side],
        )

    def load_inner():
        return pltpu.make_async_copy(
            f_hbm.at[pl.ds(1, nj - 2)], fld.at[0, pl.ds(2, nj - 2), everything, inner], local.at[4]
        )

    def load_earlier():
        return pltpu.make_async_copy(e_hbm, fld.at[1, pl.ds(1, nj), everything, inner], local.at[5])

    def load_speed():
        return pltpu.make_async_copy(c_hbm, csq, local.at[6])

    def face_copy(p, span, tile, side, sent, received):
        return pltpu.make_async_remote_copy(
            fld.at[p, 1 + (nj - 1) * side, span, tile],
            fld.at[p, (nj + 1) * (1 - side), span, tile],
            sent, received, device_id=beside("py", side), device_id_type=MESH,
        )

    def plane(p, m, side):
        return face_copy(p, span_of(m), inner, side, jsend.at[p, side], jrecv.at[p, 1 - side, m])

    def sent_planes(p, side):
        return face_copy(p, everything, inner, side, jsend.at[p, side], jrecv.at[p, 1 - side, 0])

    def last_plane(q, h, side):
        span = everything if h is None else pl.ds(1 + h * long, long)
        slot = tiles - 1 + h if q == tiles - 1 else q
        return face_copy(final, span, pl.ds(k0 + q * TILE, TILE), side, lsend.at[side], lrecv.at[1 - side, slot])

    def sent_last(side):
        return face_copy(final, everything, inner, side, lsend.at[side], lrecv.at[1 - side, 0])

    def edge_k(p, m, side):
        span = everything if m is None else span_of(m)
        return pltpu.make_async_remote_copy(
            fld.at[p, pl.ds(1, nj), span, pl.ds((k1 - 1) if side else k0, 1)],
            fld.at[p, pl.ds(1, nj), span, pl.ds((k0 - 1) if side else k1, 1)],
            ksend.at[p, side], krecv.at[p, 1 - side],
            device_id=beside("pz", side), device_id_type=MESH,
        )

    def edge_i(p, side):
        return pltpu.make_async_remote_copy(
            fld.at[p, pl.ds(1, nj), ni if side else 1, inner],
            fld.at[p, pl.ds(1, nj), 0 if side else ni + 1, inner],
            isend.at[p, side], irecv.at[p, 1 - side],
            device_id=beside("px", side), device_id_type=MESH,
        )

    def each_side(axis, do):
        for side in (0, 1):
            pl.when(has(axis, side))(functools.partial(do, side))

    def repeat(count, do, start=0):
        def body(m, _):
            do(m)
            return 0
        lax.fori_loop(start, count, body, 0)

    for part in (0, 1):
        for side in (0, 1):
            load_faces(side, part).start()

    barrier = pltpu.get_barrier_semaphore()
    expected = jnp.int32(0)
    for axis in ("py", "px", "pz"):
        for side in (0, 1):
            expected = expected + has(axis, side).astype(jnp.int32)

            @pl.when(has(axis, side))
            def _(axis=axis, side=side):
                pl.semaphore_signal(barrier, inc=1, device_id=beside(axis, side), device_id_type=MESH)

    pl.semaphore_wait(barrier, expected)

    for part, (start, stop) in enumerate(((0, 1), (1, CHUNKS))):
        for side in (0, 1):
            load_faces(side, part).wait()
        repeat(stop, lambda m: each_side("py", lambda side: plane(0, m, side).start()), start)

    load_inner().start()
    load_earlier().start()
    load_speed().start()
    load_inner().wait()
    each_side("pz", lambda side: edge_k(0, None, side).start())
    each_side("px", lambda side: edge_i(0, side).start())

    for side in (0, 1):
        @pl.when(jnp.logical_not(has("py", side)))
        def _(side=side):
            def clear(i):
                for p in (0, 1):
                    fld[p, (nj + 1) * side, i + 1, k0:k1] = jnp.zeros((nk, fld.shape[-1]), jnp.float32)
            repeat(ni, clear)

        @pl.when(jnp.logical_not(has("px", side)))
        def _(side=side):
            for p in (0, 1):
                for j in range(nj):
                    fld[p, j + 1, (ni + 1) * side, k0:k1] = jnp.zeros((nk, fld.shape[-1]), jnp.float32)

        @pl.when(jnp.logical_not(has("pz", side)))
        def _(side=side):
            at = k1 if side else k0 - 8
            def clear(i):
                for p in (0, 1):
                    for j in range(nj):
                        fld[p, j + 1, i + 1, at:at + 8] = jnp.zeros((8, fld.shape[-1]), jnp.float32)
            repeat(ni, clear)

    def later_at(p, j, i, before, middle, after, ks):
        lo, hi = k0 + ks[0], k0 + ks[1]
        along_j = fld[p, j, i, lo:hi] + fld[p, j + 2, i, lo:hi]
        along_k = fld[p, j + 1, i, lo - 1:hi - 1] + fld[p, j + 1, i, lo + 1:hi + 1]
        spread = (along_j + (before + after)) + along_k - 6.0 * middle
        return 2.0 * middle - fld[1 - p, j + 1, i, lo:hi] + csq[j, i - 1, ks[0]:ks[1]] * spread

    def sample(p, j, ks):
        i, cells = long // 2 + 1, slice(k0 + ks[0], k0 + ks[1])
        return later_at(p, j, i, fld[p, j + 1, i - 1, cells], fld[p, j + 1, i, cells], fld[p, j + 1, i + 1, cells], ks)

    def advance(p, j, first, count, ks, put, shift=None, sums=None):
        lo, hi = k0 + ks[0], k0 + ks[1]

        def row(r, carry):
            before, middle = carry[:2]
            i = first + r + 1
            after = fld[p, j + 1, i + 1, lo:hi]
            later = later_at(p, j, i, before, middle, after, ks)
            put(i - 1, later)
            if sums is None:
                return middle, after
            moved = later - shift
            return middle, after, carry[2] + moved, carry[3] + moved * moved

        carry = (fld[p, j + 1, first, lo:hi], fld[p, j + 1, first + 1, lo:hi]) + (sums or ())
        return lax.fori_loop(0, count, row, carry, unroll=4)[2:]

    def advance_faces(p, first, count, ks):
        faces, cells = (0, nj - 1), slice(k0 + ks[0], k0 + ks[1])
        shifts = [acc[f, 2] for f in range(2)]

        def row(r, carry):
            i = first + r + 1
            left = []
            for f, j in enumerate(faces):
                before, middle, total, squares = carry[4 * f:4 * f + 4]
                after = fld[p, j + 1, i + 1, cells]
                later = later_at(p, j, i, before, middle, after, ks)
                out[j, i - 1, ks[0]:ks[1]] = later
                moved = later - shifts[f]
                left += [middle, after, total + moved, squares + moved * moved]
            return tuple(left)

        carry = ()
        for f, j in enumerate(faces):
            carry += (fld[p, j + 1, first, cells], fld[p, j + 1, first + 1, cells], acc[f, 0], acc[f, 1])
        carry = lax.fori_loop(0, count, row, carry, unroll=8)
        return carry[2:4], carry[6:8]

    def with_edges(m, do):
        for side, at in ((0, 0), (1, CHUNKS - 1)):
            pl.when(jnp.logical_and(has("px", side), m == at))(functools.partial(do, side))

    for s in range(STEPS - 1):
        p, q = s % 2, 1 - s % 2
        if s == 0:
            load_earlier().wait()
            load_speed().wait()
        else:
            each_side("py", lambda side: sent_planes(q, side).wait_send())
            each_side("pz", lambda side: edge_k(q, None, side).wait_send())
            each_side("px", lambda side: edge_i(q, side).wait_send())
        each_side("pz", lambda side: edge_k(p, None, 1 - side).wait_recv())
        each_side("px", lambda side: edge_i(p, 1 - side).wait_recv())

        def chunk(m, s=s, p=p, q=q):
            each_side("py", lambda side: plane(p, m, 1 - side).wait_recv())
            for j in range(nj):
                def put(i, later, j=j):
                    fld[q, j + 1, i + 1, k0:k1] = later

                advance(p, j, m * rows, rows, (0, nk), put)
            if s < STEPS - 2:
                each_side("py", lambda side: plane(q, m, side).start())
            else:
                per = CHUNKS // SPANS

                @pl.when(lax.rem(m, per) == per - 1)
                def _():
                    each_side("py", lambda side: last_plane(0, m // per, side).start())
            each_side("pz", lambda side: edge_k(q, m, side).start())
            with_edges(m, lambda side: edge_i(q, side).start())

        repeat(CHUNKS, chunk)

    for q in range(1, tiles - 1):
        each_side("py", lambda side: last_plane(q, None, side).start())
    repeat(SPANS, lambda h: each_side("py", lambda side: last_plane(tiles - 1, h, side).start()))

    p = final
    peers = [lax.rem(x + hop, npx) for hop in range(1, npx)]

    def share(buffer, group):
        for peer in peers:
            pltpu.make_async_remote_copy(
                buffer.at[x], buffer.at[x], tsend.at[group // tiles], trecv.at[group],
                device_id={"px": peer}, device_id_type=MESH,
            ).start()

    def shared(cells, group):
        return pltpu.make_async_remote_copy(
            cells, cells, tsend.at[group // tiles], trecv.at[group], device_id={"px": peers[0]}, device_id_type=MESH
        )

    others = pl.ds(0, npx - 1)

    def local_sums(first, second, shift):
        mean = first * (1.0 / ni)
        return shift + mean, second - first * mean

    def line_sums(parts):
        mean = parts[0][0]
        for part in parts[1:]:
            mean = mean + part[0]
        mean = mean * (1.0 / npx)
        squares = jnp.zeros_like(mean)
        for part in parts:
            off = part[0] - mean
            squares = squares + (part[1] + ni * (off * off))
        return mean, lax.rsqrt(squares * (1.0 / (ni * npx)) + 0.0001)

    each_side("pz", lambda side: edge_k(p, None, 1 - side).wait_recv())
    each_side("px", lambda side: edge_i(p, 1 - side).wait_recv())
    for j in range(1, nj - 1):
        def put(i, later, j=j):
            out[j, i] = later

        shift = sample(p, j, (0, nk))
        zero = jnp.zeros_like(shift)
        sums = advance(p, j, 0, ni, (0, nk), put, shift, (zero, zero))
        inner_sums[x, 0, j - 1], inner_sums[x, 1, j - 1] = local_sums(*sums, shift)
    share(inner_sums, tiles)

    def settle_inner():
        shared(inner_sums.at[others], tiles).wait_recv()
        mean, scale = line_sums([(inner_sums[n, 0], inner_sums[n, 1]) for n in range(npx)])
        stat[0, 1:nj - 1] = mean
        stat[1, 1:nj - 1] = scale

    def settle_faces(q):
        shared(face_sums.at[q, others], q).wait_recv()
        for f, j in enumerate((0, nj - 1)):
            mean, scale = line_sums([(face_sums[q, n, 0, f], face_sums[q, n, 1, f]) for n in range(npx)])
            stat[0, j, q * TILE:(q + 1) * TILE] = mean
            stat[1, j, q * TILE:(q + 1) * TILE] = scale

    for q in range(tiles):
        ks = (q * TILE, (q + 1) * TILE)
        pieces = SPANS if q == tiles - 1 else 1
        count = ni // pieces

        def span(h, q=q, ks=ks, pieces=pieces, count=count):
            each_side("py", lambda side: last_plane(q, h if pieces > 1 else None, 1 - side).wait_recv())

            @pl.when(h == 0)
            def _():
                for f, j in enumerate((0, nj - 1)):
                    acc[f, 0] = jnp.zeros(acc.shape[2:], jnp.float32)
                    acc[f, 1] = jnp.zeros(acc.shape[2:], jnp.float32)
                    acc[f, 2] = sample(p, j, ks)

            for f, sums in enumerate(advance_faces(p, h * count, count, ks)):
                acc[f, 0], acc[f, 1] = sums

        repeat(pieces, span)
        for f in range(2):
            face_sums[q, x, 0, f], face_sums[q, x, 1, f] = local_sums(acc[f, 0], acc[f, 1], acc[f, 2])
        share(face_sums.at[q], q)
        if q == 0:
            settle_inner()
        else:
            settle_faces(q - 1)

    each_side("py", lambda side: sent_last(side).wait_send())
    each_side("py", lambda side: sent_planes(1 - p, side).wait_send())
    for t in (1 - p, p):
        each_side("pz", lambda side: edge_k(t, None, side).wait_send())
        each_side("px", lambda side: edge_i(t, side).wait_send())
    shared(inner_sums.at[others], tiles).wait_send()
    settle_faces(tiles - 1)
    shared(face_sums.at[:, others], 0).wait_send()


def normalise(f_ref, stat_ref, anomaly_hbm, end_hbm, staged, sems):
    nj, ni = f_ref.shape[:2]
    rows = ni // PARTS
    end = pltpu.make_async_copy(f_ref, end_hbm, sems.at[0])
    for j in range(nj):
        for m in range(8):
            piece = pl.ds(m * (ni // 8), ni // 8)
            pltpu.make_async_copy(f_ref.at[j, piece], end_hbm.at[j, piece], sems.at[0]).start()

    def chunk(m, _):
        for j in range(nj):
            mean, scale = stat_ref[0, j], stat_ref[1, j]

            def row(r, _):
                staged[j, m * rows + r] = (f_ref[j, m * rows + r] - mean) * scale
                return 0

            lax.fori_loop(0, rows, row, 0, unroll=4)
        piece = pl.ds(m * rows, rows)
        pltpu.make_async_copy(staged.at[:, piece], anomaly_hbm.at[:, piece], sems.at[1]).start()
        return 0

    lax.fori_loop(0, PARTS, chunk, 0)
    end.wait()
    pltpu.make_async_copy(staged, anomaly_hbm, sems.at[1]).wait()


def solution(mesh):
    npy, npx, npz = (mesh.shape[a] for a in ("py", "px", "pz"))

    def shards(field_now, earlier, speed_square):
        nj, ni, nk, nl = field_now.shape
        f32 = jnp.float32
        dma = pltpu.SemaphoreType.DMA
        hbm = pl.BlockSpec(memory_space=pltpu.HBM)
        vmem = pl.BlockSpec(memory_space=pltpu.VMEM)
        end, stat = pl.pallas_call(
            functools.partial(leapfrog, (nj, ni, nk, npy, npx, npz)),
            out_shape=(pltpu.VMEM((nj, ni, nk, nl), f32), pltpu.VMEM((2, nj, nk, nl), f32)),
            in_specs=[hbm] * 3,
            out_specs=(vmem, vmem),
            scratch_shapes=[
                pltpu.VMEM((2, nj + 2, ni + 2, nk + 2 * PAD, nl), f32),
                pltpu.VMEM((nj, ni, nk, nl), f32),
                pltpu.VMEM((2, 3, TILE, nl), f32),
                pltpu.VMEM((npx, 2, nj - 2, nk, nl), f32),
                pltpu.VMEM((nk // TILE, npx, 2, 2, TILE, nl), f32),
                dma((2, 2)), dma((2, 2, CHUNKS)),
                dma((2,)), dma((2, nk // TILE - 1 + SPANS)),
                dma((2, 2)), dma((2, 2)),
                dma((2, 2)), dma((2, 2)),
                dma((2,)), dma((nk // TILE + 1,)),
                dma((7,)),
            ],
            compiler_params=pltpu.CompilerParams(
                collective_id=0, has_side_effects=True, vmem_limit_bytes=48 << 20
            ),
            name="leapfrog",
        )(field_now, earlier, speed_square)
        return pl.pallas_call(
            normalise,
            out_shape=(jax.ShapeDtypeStruct((nj, ni, nk, nl), f32),) * 2,
            in_specs=[vmem, vmem],
            out_specs=(hbm, hbm),
            scratch_shapes=[pltpu.VMEM((nj, ni, nk, nl), f32), dma((2,))],
            compiler_params=pltpu.CompilerParams(vmem_limit_bytes=20 << 20),
            name="normalise",
        )(end, stat)

    spec = P("py", "px", "pz", None)
    return jax.shard_map(shards, mesh=mesh, in_specs=(spec,) * 3, out_specs=(spec,) * 2, check_vma=False)
```
